32 devices in a mesh: date: 4 (over y, x), pix: 8 (over z, core).
Axes of the slice: x: 2, y: 2, z: 4, core: 2. Of those that a mesh axis runs over, the one named last changes fastest.
Arguments:
- stack: bfloat16 [64, 7, 64, 1024], P('date', None, None, 'pix'), may hold values from -8 to 8
- quality: int32 [64, 64, 1024], P('date', None, 'pix'), may hold values from 0 to 1073741823
- days: int32 [64], P('date'), may hold values from 8 to 1536, as said below
Outputs:
- coef: float32 [7, 8, 64, 1024], P(None, None, 'pix', 'date')
- score: float32 [7, 64, 1024], P(None, 'pix', 'date')
The draws below stay inside these ranges and needn't reach their ends.
Inputs may be any that keep to these rules, and one draw needn't show every extreme that they name: `days`: strictly increasing.
All inputs are finite; a program needn't handle non-finite values.
Results may differ from the reference program's by a relative error of at most 0.0003.
Values may be sent and summed in bfloat16 or wider, within the bound.
No kernel may reach another device: no remote copies, remote signals or barrier semaphores. Data moves between devices by JAX's collectives and lax.ppermute only.
A program may use at most 256 MiB of HBM per device.

```python
import jax
import jax.numpy as jnp
from jax import lax

DATES = 64
BANDS = 7
HARM = 8
ROWS = 64
COLS = 1024


def make_days(key):
    inner_count = 24 * DATES - 9
    order = jax.random.permutation(jax.random.fold_in(key, 11), inner_count)
    chosen = jnp.sort(order[:DATES - 2]).astype(jnp.int32) + 9
    first = jnp.full((1,), 8, dtype=jnp.int32)
    last = jnp.full((1,), 24 * DATES, dtype=jnp.int32)
    return jnp.concatenate([first, chosen, last]).astype(jnp.int32)


def design_matrix_drawn(days):
    moment_t = days.astype(jnp.float32)
    columns = [jnp.ones_like(moment_t), (moment_t - 512.0) / 512.0]
    for order in range(1, 4):
        phase = 2.0 * jnp.pi * order * moment_t / 365.25
        columns.append(jnp.cos(phase))
        columns.append(jnp.sin(phase))
    return jnp.stack(columns, 1)


def draw_days(key, part):
    return make_days(key)


def draw_quality(key, part):
    shape = (DATES, ROWS, COLS)
    bits = jax.random.randint(jax.random.fold_in(key, 21), shape, 0, 2 ** 30)
    rows = jnp.arange(ROWS, dtype=jnp.int32)
    cols = jnp.arange(COLS, dtype=jnp.int32)
    row_limit = 300 * rows // max(ROWS - 1, 1)
    col_limit = 300 * cols // max(COLS - 1, 1)
    limit = 200 + row_limit[:, None] + col_limit[None, :]
    rolled = jax.random.randint(jax.random.fold_in(key, 22), shape, 0, 1000)
    cloud = (rolled < limit[None, :, :]).astype(jnp.int32)
    return (bits - jnp.bitwise_and(bits, 8) + 8 * cloud).astype(jnp.int32)


def draw_stack(key, part):
    design = design_matrix_drawn(make_days(key))
    coefs = 0.6 * jax.random.normal(jax.random.fold_in(key, 31), (HARM, BANDS, ROWS, COLS), jnp.float32)
    rough = jax.random.uniform(jax.random.fold_in(key, 32), (BANDS, ROWS, COLS), jnp.float32, 0.5, 1.5)
    rows = jnp.arange(ROWS, dtype=jnp.float32)
    cols = jnp.arange(COLS, dtype=jnp.float32)
    row_scale = 0.15 * jnp.power(3.2, rows / max(ROWS - 1, 1))
    col_scale = jnp.power(3.2, cols / max(COLS - 1, 1))
    scale_map = row_scale[:, None] * col_scale[None, :]
    shape = (DATES, BANDS, ROWS, COLS)
    noise = jax.random.normal(jax.random.fold_in(key, 33), shape, jnp.float32)
    signal = jnp.einsum('tk,kbrc->tbrc', design, coefs)
    values = signal + noise * rough[None] * scale_map[None, None, :, :]
    return jnp.clip(values, -8.0, 8.0).astype(jnp.bfloat16)


def setup_inputs(seed: int = 0) -> dict:
    key_of = jax.random.split(jax.random.key(seed), 4)
    stack = draw_stack(jax.random.fold_in(key_of[3], 71), 0)
    quality = draw_quality(jax.random.fold_in(key_of[3], 71), 0)
    days = draw_days(jax.random.fold_in(key_of[3], 71), 0)
    return {"stack": stack, "quality": quality, "days": days}


RIDGE_TERM = 1.0
PAIR_LIST = [(first, second) for first in range(8) for second in range(first, 8)]

def design_matrix(days):
    moment_t = days.astype(jnp.float32)
    columns = [jnp.ones_like(moment_t), (moment_t - 512.0) / 512.0]
    for order in range(1, 4):
        phase = 2.0 * jnp.pi * order * moment_t / 365.25
        columns.append(jnp.cos(phase))
        columns.append(jnp.sin(phase))
    return jnp.stack(columns, 1)

def weights(quality):
    cloud = jnp.bitwise_and(jnp.right_shift(quality, 3), 1)
    level = jnp.bitwise_and(jnp.right_shift(quality, 8), 3)
    return (1 - cloud).astype(jnp.float32) / (1.0 + level.astype(jnp.float32))

def reference(stack, quality, days):
    design = design_matrix(days)
    products = jnp.stack([design[:, first] * design[:, second] for first, second in PAIR_LIST], 1)
    index_table = [[0] * 8 for first in range(8)]
    for number, pair in enumerate(PAIR_LIST):
        index_table[pair[0]][pair[1]] = number
        index_table[pair[1]][pair[0]] = number
    index_array = jnp.array(index_table, dtype=jnp.int32)
    high = lax.Precision.HIGHEST

    def row_fit(row):
        values = lax.dynamic_slice_in_dim(stack, row, 1, 2)[:, :, 0, :].astype(jnp.float32)
        bits = lax.dynamic_slice_in_dim(quality, row, 1, 1)[:, 0, :]
        weight = weights(bits)
        gram = jnp.dot(products.T, weight, precision=high)
        moment = jnp.einsum('tk,tbc->kbc', design, weight[:, None, :] * values, precision=high)
        full = jnp.transpose(gram[index_array], (2, 0, 1)) + RIDGE_TERM * jnp.eye(8, dtype=jnp.float32)
        solved = jnp.linalg.solve(full, jnp.transpose(moment, (2, 0, 1)))
        coef_row = jnp.transpose(solved, (1, 2, 0))
        fitted = jnp.einsum('tk,kbc->tbc', design, coef_row, precision=high)
        ssr = lax.optimization_barrier(jnp.sum(weight[:, None, :] * (values - fitted) ** 2, 0))
        return (coef_row, ssr, lax.optimization_barrier(jnp.sum(weight, 0)))
    coef_rows, ssr, wsum = lax.map(row_fit, jnp.arange(ROWS, dtype=jnp.int32))
    sigma2 = lax.optimization_barrier(jnp.sum(ssr, (0, 2))) / jnp.sum(wsum)
    score = jnp.sqrt(ssr / (wsum[:, None, :] + 1.0)) / jnp.sqrt(sigma2)[None, :, None]
    return (jnp.transpose(coef_rows, (2, 1, 0, 3)), jnp.transpose(score, (1, 0, 2)))
```

```python
import functools

import jax
import jax.numpy as jnp
from jax import lax
from jax.experimental import pallas as pl
from jax.experimental.pallas import tpu as pltpu
from jax.sharding import Mesh, PartitionSpec as P


RIDGE_TERM = 1.0
HARM = 8
ROW_BLOCK = 8
LANES = 128
AXES = ("date", "q", "j")
VMEM = pl.BlockSpec(memory_space=pltpu.VMEM)
SMEM = pl.BlockSpec(memory_space=pltpu.SMEM)
THIRD = 1.0 / 3.0


def params():
    return pltpu.CompilerParams(vmem_limit_bytes=48 * 1024 * 1024)


def prep_kernel(where_ref, days_ref, stack_ref, quality_ref, *out_refs):
    dates, bands = stack_ref.shape[0], stack_ref.shape[1]
    channels = bands + 1
    lane = lax.broadcasted_iota(jnp.int32, (ROW_BLOCK, LANES), 1)
    high = jnp.zeros((ROW_BLOCK, LANES), jnp.int32)
    low = jnp.zeros((ROW_BLOCK, LANES), jnp.int32)
    for date in range(dates):
        day = days_ref[date]
        high = jnp.where(lane == date, day // 16, high)
        low = jnp.where(lane == date, day % 16, low)
    for number, out_ref in enumerate(out_refs):
        row = pl.multiple_of(where_ref[number] * ROW_BLOCK, ROW_BLOCK)
        out_ref[dates * channels] = high.astype(jnp.float32).astype(jnp.bfloat16)
        out_ref[dates * channels + 1] = low.astype(jnp.float32).astype(jnp.bfloat16)
        for date in range(dates):
            for band in range(bands):
                out_ref[date * channels + band] = stack_ref[date, band, pl.ds(row, ROW_BLOCK), :]
            bits = quality_ref[date, pl.ds(row, ROW_BLOCK), :]
            level = jnp.bitwise_and(jnp.right_shift(bits, 8), 3)
            clear = jnp.bitwise_and(bits, 8) == 0
            value = jnp.where(level < 2, jnp.where(level == 0, 1.0, 0.5), jnp.where(level == 2, THIRD, 0.25))
            out_ref[date * channels + bands] = jnp.where(clear, value, 0.0).astype(jnp.bfloat16)


def read_weight(ref, index):
    value = ref[index].astype(jnp.float32)
    third = jnp.float32(jnp.bfloat16(THIRD))
    return jnp.where(value == third, jnp.float32(THIRD), value)


def fill_design(piece_refs, dates, channels, table_ref):
    for group, ref in enumerate(piece_refs):
        high = ref[dates * channels].astype(jnp.float32)
        low = ref[dates * channels + 1].astype(jnp.float32)
        day = high * 16.0 + low
        columns = [jnp.ones_like(day), (day - 512.0) / 512.0]
        for order in range(1, 4):
            phase = 2.0 * jnp.pi * order * day / 365.25
            columns.append(jnp.cos(phase))
            columns.append(jnp.sin(phase))
        for date in range(dates):
            for i in range(1, HARM):
                table_ref[(group * dates + date) * HARM + i] = jnp.broadcast_to(
                    columns[i][:, date : date + 1], (ROW_BLOCK, LANES)
                )


def fit_kernel(groups, cores, bands, dates, *refs):
    piece_refs = refs[: groups * cores]
    coef_ref, table_ref, gram_ref, moment_ref = refs[groups * cores :]
    channels = bands + 1
    fill_design([piece_refs[g * cores] for g in range(groups)], dates, channels, table_ref)
    zero = jnp.zeros((ROW_BLOCK, LANES), jnp.float32)
    pairs = [(i, j) for i in range(HARM) for j in range(i, HARM)]

    def columns_of(line):
        return [None] + [table_ref[line * HARM + i] for i in range(1, HARM)]

    for core in range(cores):
        totals = [zero] * len(pairs)
        for group in range(groups):
            ref = piece_refs[group * cores + core]

            def gram_step(date, totals):
                d = columns_of(group * dates + date)
                w = read_weight(ref, date * channels + bands)
                wd = [w] + [w * d[i] for i in range(1, HARM)]
                return [t + (wd[j] if i == 0 else wd[i] * d[j]) for t, (i, j) in zip(totals, pairs)]

            totals = lax.fori_loop(0, dates, gram_step, totals)
        for number, total in enumerate(totals):
            gram_ref[number] = total
        for first in range(0, bands, 4):
            some = range(first, min(first + 4, bands))
            totals = [zero] * (len(some) * HARM)
            for group in range(groups):
                ref = piece_refs[group * cores + core]

                def moment_step(date, totals):
                    d = columns_of(group * dates + date)
                    w = read_weight(ref, date * channels + bands)
                    out = []
                    for number, band in enumerate(some):
                        wy = w * ref[date * channels + band].astype(jnp.float32)
                        for i in range(HARM):
                            out.append(totals[number * HARM + i] + (wy if i == 0 else wy * d[i]))
                    return out

                totals = lax.fori_loop(0, dates, moment_step, totals)
            for number, band in enumerate(some):
                for i in range(HARM):
                    moment_ref[band * HARM + i] = totals[number * HARM + i]
        lower, scaled, inverse = {}, {}, []
        for j in range(HARM):
            for i in range(j, HARM):
                total = gram_ref[pairs.index((j, i))]
                if i == j:
                    total = total + RIDGE_TERM
                for k in range(j):
                    total = total - lower[i, k] * scaled[j, k]
                if i == j:
                    inverse.append(1.0 / total)
                else:
                    scaled[i, j] = total
            for i in range(j + 1, HARM):
                lower[i, j] = scaled[i, j] * inverse[j]
        for band in range(bands):
            x = []
            for i in range(HARM):
                total = moment_ref[band * HARM + i]
                for k in range(i):
                    total = total - lower[i, k] * x[k]
                x.append(total)
            x = [v * inverse[i] for i, v in enumerate(x)]
            for i in range(HARM - 1, -1, -1):
                for k in range(i + 1, HARM):
                    x[i] = x[i] - lower[k, i] * x[k]
            for i in range(HARM):
                coef_ref[core, band * HARM + i] = x[i]


def residual_kernel(groups, cores, bands, dates, devices, *refs):
    piece_refs = refs[: groups * cores]
    coef_ref, table_ref, score_ref, sums_ref = refs[groups * cores :]
    channels = bands + 1
    zero = jnp.zeros((ROW_BLOCK, LANES), jnp.float32)
    ssr_sum, weight_sum = [zero] * bands, zero
    for core in range(cores):
        wsum = zero
        for first in range(0, bands, 4):
            some = range(first, min(first + 4, bands))
            coefs = [[coef_ref[core, band * HARM + i] for i in range(HARM)] for band in some]
            totals = [zero] * (len(some) + 1)
            for group in range(groups):
                ref = piece_refs[group * cores + core]

                def step(date, totals):
                    d = [None] + [table_ref[((group * dates) + date) * HARM + i] for i in range(1, HARM)]
                    w = read_weight(ref, date * channels + bands)
                    out = []
                    for number, band in enumerate(some):
                        c = coefs[number]
                        f = c[0]
                        for i in range(1, HARM):
                            f = f + c[i] * d[i]
                        r = ref[date * channels + band].astype(jnp.float32) - f
                        out.append(totals[number] + w * (r * r))
                    return out + [totals[-1] + w]

                totals = lax.fori_loop(0, dates, step, totals)
            wsum = totals[-1]
            for number, band in enumerate(some):
                ssr_sum[band] = ssr_sum[band] + totals[number]
                score_ref[core, band] = jnp.sqrt(totals[number] / (wsum + 1.0))
        weight_sum = weight_sum + wsum
    lane = lax.broadcasted_iota(jnp.int32, (devices, LANES), 1)
    sums = jnp.zeros((devices, LANES), jnp.float32)
    for number, total in enumerate(ssr_sum + [weight_sum]):
        sums = jnp.where(lane == number, jnp.sum(total), sums)
    sums_ref[...] = sums


def final_kernel(cores, bands, where_ref, sums_ref, coef_ref, score_ref, coef_out_ref, score_out_ref):
    total = jnp.sum(sums_ref[...], 0, keepdims=True)
    weight = total[:, bands : bands + 1]
    for block in range(cores):
        columns = pl.ds(block * LANES, LANES)
        source = where_ref[block]
        for band in range(bands):
            factor = 1.0 / jnp.sqrt(total[:, band : band + 1] / weight)
            score_out_ref[band, :, columns] = score_ref[source, band] * factor
            for i in range(HARM):
                coef_out_ref[band, i, :, columns] = coef_ref[source, band * HARM + i]


def local(groups, cores, stack, quality, days):
    dates, bands = stack.shape[0], stack.shape[1]
    devices = groups * groups * cores
    channels = bands + 1
    tiles = dates * channels + 2
    me_d, me_q, me_j = (lax.axis_index(name) for name in AXES)

    def device(d, q, j):
        return (d * groups + q) * cores + j

    def turn(q, j):
        return q ^ ((j % 2) * (groups // 2))

    every = [(d, q, j) for d in range(groups) for q in range(groups) for j in range(cores)]
    relations = [(kd, kj) for kd in range(groups) for kj in range(cores)]
    rows = jnp.stack([((me_d ^ kd) ^ turn(me_q, me_j)) * cores + (me_j ^ kj) for kd, kj in relations])
    pieces = pl.pallas_call(
        prep_kernel,
        out_shape=[jax.ShapeDtypeStruct((tiles, ROW_BLOCK, LANES), jnp.bfloat16)] * len(relations),
        in_specs=[SMEM, SMEM, VMEM, VMEM],
        out_specs=[VMEM] * len(relations),
        compiler_params=params(),
        name="prep",
    )(rows.astype(jnp.int32), days, stack, quality)
    got = []
    for (kd, kj), piece in zip(relations, pieces):
        if kd or kj:
            piece = lax.ppermute(
                piece, AXES, [(device(d, q, j), device(d ^ kd, q, j ^ kj)) for d, q, j in every]
            )
        got.append(piece)
    block = (ROW_BLOCK, LANES)
    coef, table = pl.pallas_call(
        lambda *refs: fit_kernel(groups, cores, bands, dates, *refs),
        out_shape=[
            jax.ShapeDtypeStruct((cores, bands * HARM) + block, jnp.float32),
            jax.ShapeDtypeStruct((groups * dates * HARM,) + block, jnp.float32),
        ],
        in_specs=[VMEM] * len(got),
        out_specs=[VMEM] * 2,
        scratch_shapes=[
            pltpu.VMEM((HARM * (HARM + 1) // 2,) + block, jnp.float32),
            pltpu.VMEM((bands * HARM,) + block, jnp.float32),
        ],
        compiler_params=params(),
        name="fit",
    )(*got)
    score, sums = pl.pallas_call(
        lambda *refs: residual_kernel(groups, cores, bands, dates, devices, *refs),
        out_shape=[
            jax.ShapeDtypeStruct((cores, bands) + block, jnp.float32),
            jax.ShapeDtypeStruct((devices, LANES), jnp.float32),
        ],
        in_specs=[VMEM] * (len(got) + 2),
        out_specs=[VMEM] * 2,
        compiler_params=params(),
        name="residual",
    )(*got, coef, table)

    def deliver(values):
        parts = []
        for slot in range(cores):
            parts.append(
                lax.ppermute(
                    values[slot],
                    AXES,
                    [(device(d, q, j), device(q, d ^ turn(q, j ^ slot), j)) for d, q, j in every],
                )
            )
        return jnp.stack(parts)

    coef = deliver(coef)
    score = deliver(score)
    sums = lax.all_to_all(sums, AXES, 0, 0, tiled=True)
    order = jnp.stack([me_j ^ number for number in range(cores)]).astype(jnp.int32)
    return pl.pallas_call(
        lambda *refs: final_kernel(cores, bands, *refs),
        out_shape=[
            jax.ShapeDtypeStruct((bands, HARM, ROW_BLOCK, cores * LANES), jnp.float32),
            jax.ShapeDtypeStruct((bands, ROW_BLOCK, cores * LANES), jnp.float32),
        ],
        in_specs=[SMEM, VMEM, VMEM, VMEM],
        out_specs=[VMEM] * 2,
        compiler_params=params(),
        name="final",
    )(order, sums, coef, score)


def solution(mesh):
    groups, across = mesh.shape["date"], mesh.shape["pix"]
    cores = across // groups
    split = Mesh(mesh.devices.reshape(groups, groups, cores), AXES)
    return jax.shard_map(
        functools.partial(local, groups, cores),
        mesh=split,
        in_specs=(
            P("date", None, None, ("q", "j")),
            P("date", None, ("q", "j")),
            P("date"),
        ),
        out_specs=(P(None, None, ("q", "j"), "date"), P(None, ("q", "j"), "date")),
        check_vma=False,
    )
```

```python
import functools

import jax
import jax.numpy as jnp
from jax import lax
from jax.experimental import pallas as pl
from jax.experimental.pallas import tpu as pltpu
from jax.sharding import Mesh, PartitionSpec as P


RIDGE_TERM = 1.0
HARM = 8
PAIRS = [(i, j) for i in range(HARM) for j in range(i, HARM)]
ROWS = 8
LANES = 128
TILE = (ROWS, LANES)
AXES = ("date", "q", "j")
VMEM = pl.BlockSpec(memory_space=pltpu.VMEM)
SMEM = pl.BlockSpec(memory_space=pltpu.SMEM)
HBM = pl.BlockSpec(memory_space=pltpu.HBM)
THIRD = 1.0 / 3.0


def params(spare=16):
    return pltpu.CompilerParams(vmem_limit_bytes=67043328 - spare * 1024 * 1024)


def f32(*shape):
    return jax.ShapeDtypeStruct(shape, jnp.float32)


def turn(groups, q, j):
    return q ^ ((j % 2) * (groups // 2))


def prep_kernel(order, days_ref, stack_ref, quality_ref, *refs):
    *out_refs, bits_ref, sem, bits_sem = refs
    dates, bands = stack_ref.shape[0], stack_ref.shape[1]
    blocks = out_refs[0].shape[1] // ROWS
    me_d, me_q, me_j = (lax.axis_index(name) for name in AXES)

    def spot(kd, block):
        group = ((me_d ^ kd) ^ turn(len(order), me_q, me_j)) * blocks + (me_j ^ block)
        return pl.ds(pl.multiple_of(group * ROWS, ROWS), ROWS)

    fetch = pltpu.make_async_copy(quality_ref, bits_ref, bits_sem)
    fetch.start()
    copies = []
    for number in order:
        for block in range(blocks):
            for band in range(bands):
                copy = pltpu.make_async_copy(
                    stack_ref.at[:, band, spot(number, block), :],
                    out_refs[number].at[pl.ds(band * dates, dates), pl.ds(block * ROWS, ROWS)],
                    sem.at[number, block, band],
                )
                copy.start()
                copies.append(copy)
    lane = lax.broadcasted_iota(jnp.int32, TILE, 1)
    high = jnp.zeros(TILE, jnp.int32)
    low = jnp.zeros(TILE, jnp.int32)
    for date in range(dates):
        day = days_ref[date]
        high = jnp.where(lane == date, day // 16, high)
        low = jnp.where(lane == date, day % 16, low)
    high = high.astype(jnp.float32).astype(jnp.bfloat16)
    low = low.astype(jnp.float32).astype(jnp.bfloat16)
    fetch.wait()
    for number in order:
        out_ref = out_refs[number]
        out_ref[dates * (bands + 1), pl.ds(0, ROWS)] = high
        out_ref[dates * (bands + 1), pl.ds(ROWS, ROWS)] = low
        for date in range(dates):
            for block in range(blocks):
                bits = bits_ref[date, spot(number, block), :]
                level = jnp.bitwise_and(jnp.right_shift(bits, 8), 3)
                clear = jnp.bitwise_and(bits, 8) == 0
                value = jnp.where(level < 2, jnp.where(level == 0, 1.0, 0.5), jnp.where(level == 2, THIRD, 0.25))
                value = jnp.where(clear, value, 0.0).astype(jnp.bfloat16)
                out_ref[dates * bands + date, pl.ds(block * ROWS, ROWS)] = value
    for copy in copies:
        copy.wait()


def tile_of(ref, index, block):
    return ref[index, pl.ds(block * ROWS, ROWS), :].astype(jnp.float32)


def tables(dates, bands, blocks, piece_ref, table_ref, weight_ref):
    high = tile_of(piece_ref, dates * (bands + 1), 0)
    low = tile_of(piece_ref, dates * (bands + 1), 1)
    day = high * 16.0 + low
    columns = [None, (day - 512.0) / 512.0]
    for order in range(1, 4):
        phase = 2.0 * jnp.pi * order * day / 365.25
        columns.append(jnp.cos(phase))
        columns.append(jnp.sin(phase))
    for date in range(dates):
        for i in range(1, HARM):
            table_ref[date * HARM + i] = jnp.broadcast_to(columns[i][:, date : date + 1], TILE)
    third = jnp.float32(jnp.bfloat16(THIRD))
    for block in range(blocks):
        for date in range(dates):
            value = tile_of(piece_ref, dates * bands + date, block)
            weight_ref[block * dates + date] = jnp.where(value == third, jnp.float32(THIRD), value)


def band_sets(bands):
    return [range(first, min(first + 4, bands)) for first in range(0, bands, 4)]


def add_sums(dates, bands, blocks, piece_ref, table_ref, weight_ref, old, new):
    zero = jnp.zeros(TILE, jnp.float32)
    for block in range(blocks):

        def gram_step(date, totals):
            d = [None] + [table_ref[date * HARM + i] for i in range(1, HARM)]
            w = weight_ref[block * dates + date]
            wd = [w] + [w * d[i] for i in range(1, HARM)]
            return [t + (wd[j] if i == 0 else wd[i] * d[j]) for t, (i, j) in zip(totals, PAIRS)]

        start = [zero if old is None else old[0][block, n] for n in range(len(PAIRS))]
        for n, total in enumerate(lax.fori_loop(0, dates, gram_step, start, unroll=2)):
            new[0][block, n] = total
        for some in band_sets(bands):

            def moment_step(date, totals):
                d = [None] + [table_ref[date * HARM + i] for i in range(1, HARM)]
                w = weight_ref[block * dates + date]
                out = []
                for n, band in enumerate(some):
                    wy = w * tile_of(piece_ref, band * dates + date, block)
                    for i in range(HARM):
                        out.append(totals[n * HARM + i] + (wy if i == 0 else wy * d[i]))
                return out

            places = [band * HARM + i for band in some for i in range(HARM)]
            start = [zero if old is None else old[1][block, n] for n in places]
            for n, total in zip(places, lax.fori_loop(0, dates, moment_step, start, unroll=2)):
                new[1][block, n] = total


def first_kernel(dates, bands, blocks, piece_ref, gram_ref, moment_ref, table_ref, weight_ref):
    tables(dates, bands, blocks, piece_ref, table_ref, weight_ref)
    add_sums(dates, bands, blocks, piece_ref, table_ref, weight_ref, None, (gram_ref, moment_ref))


def more_kernel(dates, bands, blocks, piece_ref, old_gram, old_moment, gram_ref, moment_ref, table_ref, weight_ref):
    tables(dates, bands, blocks, piece_ref, table_ref, weight_ref)
    add_sums(dates, bands, blocks, piece_ref, table_ref, weight_ref, (old_gram, old_moment), (gram_ref, moment_ref))


def solve(bands, gram, moment, put):
    lower, scaled, inverse = {}, {}, []
    for j in range(HARM):
        for i in range(j, HARM):
            total = gram(PAIRS.index((j, i)))
            if i == j:
                total = total + RIDGE_TERM
            for k in range(j):
                total = total - lower[i, k] * scaled[j, k]
            if i == j:
                inverse.append(1.0 / total)
            else:
                scaled[i, j] = total
        for i in range(j + 1, HARM):
            lower[i, j] = scaled[i, j] * inverse[j]
    for band in range(bands):
        x = []
        for i in range(HARM):
            total = moment(band * HARM + i)
            for k in range(i):
                total = total - lower[i, k] * x[k]
            x.append(total)
        x = [v * inverse[i] for i, v in enumerate(x)]
        for i in range(HARM - 1, -1, -1):
            for k in range(i + 1, HARM):
                x[i] = x[i] - lower[k, i] * x[k]
            put(band * HARM + i, x[i])


def last_kernel(groups, dates, bands, blocks, devices, last, *refs):
    piece_refs, refs = refs[:groups], refs[groups:]
    table_refs, refs = list(refs[: groups - 1]), refs[groups - 1 :]
    weight_refs, refs = list(refs[: groups - 1]), refs[groups - 1 :]
    old_gram, old_moment, *out_refs, sums_ref, gram_ref, moment_ref, table_ref, weight_ref = refs
    table_refs.append(table_ref)
    weight_refs.append(weight_ref)
    tables(dates, bands, blocks, piece_refs[-1], table_ref, weight_ref)
    add_sums(
        dates, bands, blocks, piece_refs[-1], table_ref, weight_ref,
        (old_gram, old_moment), (gram_ref, moment_ref),
    )
    zero = jnp.zeros(TILE, jnp.float32)
    ssr_sum, weight_sum = [zero] * bands, zero
    for block, out_ref in enumerate(out_refs):

        def put(number, value):
            out_ref[number] = value

        solve(bands, lambda n: gram_ref[block, n], lambda n: moment_ref[block, n], put)
        wsum = gram_ref[block, 0]
        weight_sum = weight_sum + wsum
        for some in band_sets(bands):
            coefs = [[out_ref[band * HARM + i] for i in range(HARM)] for band in some]
            totals = [zero] * len(some)
            for piece_ref, table_ref, weight_ref in zip(piece_refs, table_refs, weight_refs):

                def step(date, totals):
                    d = [None] + [table_ref[date * HARM + i] for i in range(1, HARM)]
                    w = weight_ref[block * dates + date]
                    out = []
                    for n, band in enumerate(some):
                        c = coefs[n]
                        y = tile_of(piece_ref, band * dates + date, block)
                        r = ((y - c[0]) - (c[1] * d[1] + c[2] * d[2])) - (
                            (c[3] * d[3] + c[4] * d[4]) + ((c[5] * d[5] + c[6] * d[6]) + c[7] * d[7])
                        )
                        out.append(totals[n] + w * (r * r))
                    return out

                totals = lax.fori_loop(0, dates, step, totals, unroll=2)
            for n, band in enumerate(some):
                ssr_sum[band] = ssr_sum[band] + totals[n]
                out_ref[bands * HARM + band] = jnp.sqrt(totals[n] / (wsum + 1.0))
    lane = lax.broadcasted_iota(jnp.int32, (devices, LANES), 1)
    sums = jnp.zeros((devices, LANES), jnp.float32)
    for number, total in enumerate(ssr_sum + [weight_sum]):
        sums = jnp.where(lane == number, jnp.sum(total), sums)
    sums_ref[...] = sums


def final_kernel(cores, bands, sums_ref, *refs):
    me_j = lax.axis_index("j")
    got_refs, (coef_ref, score_ref, sem) = refs[:cores], refs[cores:]
    copies = []
    for slot in range(cores):
        columns = pl.ds(pl.multiple_of((me_j ^ slot) * LANES, LANES), LANES)
        for band in range(bands):
            copy = pltpu.make_async_copy(
                got_refs[slot].at[pl.ds(band * HARM, HARM)], coef_ref.at[band, :, :, columns], sem.at[slot, band]
            )
            copy.start()
            copies.append(copy)
    total = jnp.sum(sums_ref[...], 0, keepdims=True)
    weight = total[:, bands : bands + 1]
    for band in range(bands):
        factor = 1.0 / jnp.sqrt(total[:, band : band + 1] / weight)
        for slot in range(cores):
            columns = pl.ds(pl.multiple_of((me_j ^ slot) * LANES, LANES), LANES)
            score_ref[band, :, columns] = got_refs[slot][bands * HARM + band] * factor
    for copy in copies:
        copy.wait()


def local(groups, cores, stack, quality, days):
    dates, bands = stack.shape[0], stack.shape[1]
    devices = groups * groups * cores

    def device(d, q, j):
        return (d * groups + q) * cores + j

    every = [(d, q, j) for d in range(groups) for q in range(groups) for j in range(cores)]
    order = sorted(range(groups), key=lambda kd: -bin(kd).count("1"))
    slabs = dates * (bands + 1) + 1
    piece = jax.ShapeDtypeStruct((slabs, cores * ROWS, LANES), jnp.bfloat16)
    pieces = pl.pallas_call(
        functools.partial(prep_kernel, order),
        out_shape=[piece] * groups,
        in_specs=[SMEM, HBM, HBM],
        out_specs=[VMEM] * groups,
        scratch_shapes=[
            pltpu.VMEM(quality.shape, jnp.int32),
            pltpu.SemaphoreType.DMA((groups, cores, bands)),
            pltpu.SemaphoreType.DMA,
        ],
        compiler_params=params(3),
        name="prep",
    )(days, stack, quality)
    got = []
    for kd in order:
        if kd:
            got.append(
                lax.ppermute(pieces[kd], AXES, [(device(d, q, j), device(d ^ kd, q, j)) for d, q, j in every])
            )
    got = [pieces[0]] + got
    gram, moment = f32(cores, len(PAIRS), *TILE), f32(cores, bands * HARM, *TILE)
    table, weight = f32(dates * HARM, *TILE), f32(cores * dates, *TILE)
    sizes = (dates, bands, cores)
    cost = pl.CostEstimate(flops=2 * 100 * dates * cores * ROWS * LANES * 8, bytes_accessed=1 << 20, transcendentals=0)
    table_list, weight_list = [], []
    sums = None
    for number in range(groups - 1):
        kernel = first_kernel if number == 0 else more_kernel
        given = [got[number]] + ([] if number == 0 else list(sums))
        *sums, t, w = pl.pallas_call(
            functools.partial(kernel, *sizes),
            out_shape=[gram, moment, table, weight],
            in_specs=[VMEM] * len(given),
            out_specs=[VMEM] * 4,
            compiler_params=params(),
            cost_estimate=cost,
            name="sums%d" % number,
        )(*given)
        table_list.append(t)
        weight_list.append(w)
    given = got + table_list + weight_list + list(sums)
    *fitted, totals = pl.pallas_call(
        functools.partial(last_kernel, groups, *sizes, devices, groups - 1),
        out_shape=[f32(bands * (HARM + 1), *TILE)] * cores + [f32(devices, LANES)],
        in_specs=[VMEM] * len(given),
        out_specs=[VMEM] * (cores + 1),
        scratch_shapes=[pltpu.VMEM(s.shape, s.dtype) for s in (gram, moment, table, weight)],
        compiler_params=params(),
        cost_estimate=cost,
        name="last",
    )(*given)
    moved = []
    for slot in range(cores):
        moved.append(
            lax.ppermute(
                fitted[slot], AXES, [(device(d, q, j), device(q, d ^ turn(groups, q, j), j ^ slot)) for d, q, j in every]
            )
        )
    totals = lax.all_to_all(totals, AXES, 0, 0, tiled=True)
    return pl.pallas_call(
        functools.partial(final_kernel, cores, bands),
        out_shape=[f32(bands, HARM, ROWS, cores * LANES), f32(bands, ROWS, cores * LANES)],
        in_specs=[VMEM] * (1 + cores),
        out_specs=[HBM, VMEM],
        scratch_shapes=[pltpu.SemaphoreType.DMA((cores, bands))],
        compiler_params=params(),
        name="final",
    )(totals, *moved)


def solution(mesh):
    groups, across = mesh.shape["date"], mesh.shape["pix"]
    cores = across // groups
    split = Mesh(mesh.devices.reshape(groups, groups, cores), AXES)
    return jax.shard_map(
        functools.partial(local, groups, cores),
        mesh=split,
        in_specs=(
            P("date", None, None, ("q", "j")),
            P("date", None, ("q", "j")),
            P("date"),
        ),
        out_specs=(P(None, None, ("q", "j"), "date"), P(None, ("q", "j"), "date")),
        check_vma=False,
    )
```

```python
import functools

import jax
import jax.numpy as jnp
from jax import lax
from jax.experimental import pallas as pl
from jax.experimental.pallas import tpu as pltpu
from jax.sharding import Mesh, PartitionSpec as P


RIDGE_TERM = 1.0
HARM = 8
PAIRS = [(i, j) for i in range(HARM) for j in range(i, HARM)]
ROWS = 8
LANES = 128
TILE = (ROWS, LANES)
AXES = ("date", "q", "j")
VMEM = pl.BlockSpec(memory_space=pltpu.VMEM)
SMEM = pl.BlockSpec(memory_space=pltpu.SMEM)
HBM = pl.BlockSpec(memory_space=pltpu.HBM)
THIRD = 1.0 / 3.0
PREP_SPARE = (11, 11)


def params(spare=16):
    return pltpu.CompilerParams(vmem_limit_bytes=67043328 - spare * 1024 * 1024)


def f32(*shape):
    return jax.ShapeDtypeStruct(shape, jnp.float32)


def turn(groups, q, j):
    return q ^ ((j % 2) * (groups // 2))


def prep_kernel(groups, cores, slots, with_days, days_ref, stack_ref, quality_ref, *refs):
    *out_refs, bits_ref, sem, bits_sem = refs
    dates, bands = stack_ref.shape[0], stack_ref.shape[1]
    me_d, me_q, me_j = (lax.axis_index(name) for name in AXES)

    def spot(kd, slot):
        group = ((me_d ^ kd) ^ turn(groups, me_q, me_j)) * cores + (me_j ^ slot)
        return pl.ds(pl.multiple_of(group * ROWS, ROWS), ROWS)

    copies, fetches = [], []
    for kd in range(groups):
        for block, slot in enumerate(slots):
            fetches.append(
                pltpu.make_async_copy(
                    quality_ref.at[:, spot(kd, slot), :], bits_ref.at[kd, block], bits_sem.at[kd, block]
                )
            )
            fetches[-1].start()
    for kd in range(groups):
        for block, slot in enumerate(slots):
            for band in range(bands):
                copies.append(
                    pltpu.make_async_copy(
                        stack_ref.at[:, band, spot(kd, slot), :],
                        out_refs[kd].at[pl.ds(band * dates, dates), pl.ds(block * ROWS, ROWS)],
                        sem.at[kd, block, band],
                    )
                )
                copies[-1].start()
    if with_days:
        lane = lax.broadcasted_iota(jnp.int32, TILE, 1)
        high = jnp.zeros(TILE, jnp.int32)
        low = jnp.zeros(TILE, jnp.int32)
        for date in range(dates):
            day = days_ref[date]
            high = jnp.where(lane == date, day // 16, high)
            low = jnp.where(lane == date, day % 16, low)
        for kd in range(groups):
            for n, part in enumerate((high, low)):
                out_refs[kd][dates * (bands + 1) + n, pl.ds(0, ROWS)] = part.astype(jnp.float32).astype(jnp.bfloat16)
    for fetch in fetches:
        fetch.wait()
    for kd in range(groups):
        for block in range(len(slots)):
            for date in range(dates):
                bits = bits_ref[kd, block, date]
                level = jnp.bitwise_and(jnp.right_shift(bits, 8), 3)
                clear = jnp.bitwise_and(bits, 8) == 0
                value = jnp.where(level < 2, jnp.where(level == 0, 1.0, 0.5), jnp.where(level == 2, THIRD, 0.25))
                value = jnp.where(clear, value, 0.0).astype(jnp.bfloat16)
                out_refs[kd][dates * bands + date, pl.ds(block * ROWS, ROWS)] = value
    for copy in copies:
        copy.wait()


def tile_of(ref, index, block):
    return ref[index, pl.ds(block * ROWS, ROWS), :].astype(jnp.float32)


def fill_table(dates, bands, piece_ref, table_ref):
    high = tile_of(piece_ref, dates * (bands + 1), 0)
    low = tile_of(piece_ref, dates * (bands + 1) + 1, 0)
    day = high * 16.0 + low
    columns = [None, (day - 512.0) / 512.0]
    for order in range(1, 4):
        phase = 2.0 * jnp.pi * order * day / 365.25
        columns.append(jnp.cos(phase))
        columns.append(jnp.sin(phase))
    for date in range(dates):
        for i in range(1, HARM):
            table_ref[date * HARM + i] = jnp.broadcast_to(columns[i][:, date : date + 1], TILE)


def fill_weight(dates, bands, blocks, piece_ref, weight_ref):
    third = jnp.float32(jnp.bfloat16(THIRD))
    for block in range(blocks):
        for date in range(dates):
            value = tile_of(piece_ref, dates * bands + date, block)
            weight_ref[block * dates + date] = jnp.where(value == third, jnp.float32(THIRD), value)


def band_sets(bands):
    return [range(first, min(first + 4, bands)) for first in range(0, bands, 4)]


def add_sums(dates, bands, blocks, piece_ref, table_ref, weight_ref, old, new):
    zero = jnp.zeros(TILE, jnp.float32)
    for block in range(blocks):

        def gram_step(date, totals):
            d = [None] + [table_ref[date * HARM + i] for i in range(1, HARM)]
            w = weight_ref[block * dates + date]
            wd = [w] + [w * d[i] for i in range(1, HARM)]
            return [t + (wd[j] if i == 0 else wd[i] * d[j]) for t, (i, j) in zip(totals, PAIRS)]

        start = [zero if old is None else old[0][block, n] for n in range(len(PAIRS))]
        for n, total in enumerate(lax.fori_loop(0, dates, gram_step, start, unroll=2)):
            new[0][block, n] = total
        for some in band_sets(bands):

            def moment_step(date, totals):
                d = [None] + [table_ref[date * HARM + i] for i in range(1, HARM)]
                w = weight_ref[block * dates + date]
                out = []
                for n, band in enumerate(some):
                    wy = w * tile_of(piece_ref, band * dates + date, block)
                    for i in range(HARM):
                        out.append(totals[n * HARM + i] + (wy if i == 0 else wy * d[i]))
                return out

            places = [band * HARM + i for band in some for i in range(HARM)]
            start = [zero if old is None else old[1][block, n] for n in places]
            for n, total in zip(places, lax.fori_loop(0, dates, moment_step, start, unroll=2)):
                new[1][block, n] = total


def solve(bands, gram, moment, put):
    lower, scaled, inverse = {}, {}, []
    for j in range(HARM):
        for i in range(j, HARM):
            total = gram(PAIRS.index((j, i)))
            if i == j:
                total = total + RIDGE_TERM
            for k in range(j):
                total = total - lower[i, k] * scaled[j, k]
            if i == j:
                inverse.append(1.0 / total)
            else:
                scaled[i, j] = total
        for i in range(j + 1, HARM):
            lower[i, j] = scaled[i, j] * inverse[j]
    for band in range(bands):
        x = []
        for i in range(HARM):
            total = moment(band * HARM + i)
            for k in range(i):
                total = total - lower[i, k] * x[k]
            x.append(total)
        x = [v * inverse[i] for i, v in enumerate(x)]
        for i in range(HARM - 1, -1, -1):
            for k in range(i + 1, HARM):
                x[i] = x[i] - lower[k, i] * x[k]
            put(band * HARM + i, x[i])


def part_kernel(sizes, names, *refs):
    dates, bands, blocks, _ = sizes
    refs = dict(zip(names, refs, strict=True))

    def some(kind):
        return [refs[name] for name in names if name.startswith(kind + ".")]

    new, table, weight = some("new"), some("table"), some("weight")
    for number, (piece_ref, weight_ref) in enumerate(zip(new, weight)):
        if some("made"):
            fill_table(dates, bands, piece_ref, some("made")[number])
        fill_weight(dates, bands, blocks, piece_ref, weight_ref)
    table = some("made") or table
    old = (refs["in_gram"], refs["in_moment"]) if "in_gram" in refs else None
    sums = (refs["gram"], refs["moment"])
    for piece_ref, table_ref, weight_ref in zip(new, table, weight):
        add_sums(dates, bands, blocks, piece_ref, table_ref, weight_ref, old, sums)
        old = sums
    if "totals" in refs:
        finish(
            sizes,
            some("was") + new, some("was_table") + table, some("was_weight") + weight,
            sums, some("out"), refs.get("in_totals"), refs["totals"],
        )


def finish(sizes, piece_refs, table_refs, weight_refs, sums, out_refs, before_ref, totals_ref):
    dates, bands, _, devices = sizes
    zero = jnp.zeros(TILE, jnp.float32)
    ssr_sum, weight_sum = [zero] * bands, zero
    for block, out_ref in enumerate(out_refs):

        def put(number, value):
            out_ref[number] = value

        solve(bands, lambda n: sums[0][block, n], lambda n: sums[1][block, n], put)
        wsum = sums[0][block, 0]
        weight_sum = weight_sum + wsum
        for some in band_sets(bands):
            coefs = [[out_ref[band * HARM + i] for i in range(HARM)] for band in some]
            totals = [zero] * len(some)
            for piece_ref, table_ref, weight_ref in zip(piece_refs, table_refs, weight_refs, strict=True):

                def step(date, totals):
                    d = [None] + [table_ref[date * HARM + i] for i in range(1, HARM)]
                    w = weight_ref[block * dates + date]
                    out = []
                    for n, band in enumerate(some):
                        c = coefs[n]
                        y = tile_of(piece_ref, band * dates + date, block)
                        r = ((y - c[0]) - (c[1] * d[1] + c[2] * d[2])) - (
                            (c[3] * d[3] + c[4] * d[4]) + ((c[5] * d[5] + c[6] * d[6]) + c[7] * d[7])
                        )
                        out.append(totals[n] + w * (r * r))
                    return out

                totals = lax.fori_loop(0, dates, step, totals, unroll=2)
            for n, band in enumerate(some):
                ssr_sum[band] = ssr_sum[band] + totals[n]
                out_ref[bands * HARM + band] = jnp.sqrt(totals[n] / (wsum + 1.0))
    if before_ref is not None:
        ssr_sum = [total + before_ref[band] for band, total in enumerate(ssr_sum)]
        weight_sum = weight_sum + before_ref[bands]
    if len(totals_ref.shape) == 3:
        for number, total in enumerate(ssr_sum + [weight_sum]):
            totals_ref[number] = total
        return
    lane = lax.broadcasted_iota(jnp.int32, (devices, LANES), 1)
    sums = jnp.zeros((devices, LANES), jnp.float32)
    for number, total in enumerate(ssr_sum + [weight_sum]):
        sums = jnp.where(lane == number, jnp.sum(total), sums)
    totals_ref[...] = sums


def final_kernel(cores, bands, sums_ref, *refs):
    me_j = lax.axis_index("j")
    got_refs, (coef_ref, score_ref, sem) = refs[:cores], refs[cores:]
    copies = []
    for slot in range(cores):
        columns = pl.ds(pl.multiple_of((me_j ^ slot) * LANES, LANES), LANES)
        for band in range(bands):
            copy = pltpu.make_async_copy(
                got_refs[slot].at[pl.ds(band * HARM, HARM)], coef_ref.at[band, :, :, columns], sem.at[slot, band]
            )
            copy.start()
            copies.append(copy)
    total = jnp.sum(sums_ref[...], 0, keepdims=True)
    weight = total[:, bands : bands + 1]
    for band in range(bands):
        factor = 1.0 / jnp.sqrt(total[:, band : band + 1] / weight)
        for slot in range(cores):
            columns = pl.ds(pl.multiple_of((me_j ^ slot) * LANES, LANES), LANES)
            score_ref[band, :, columns] = got_refs[slot][bands * HARM + band] * factor
    for copy in copies:
        copy.wait()


def local(groups, cores, stack, quality, days):
    dates, bands = stack.shape[0], stack.shape[1]
    devices = groups * groups * cores
    half = cores // 2
    phases = [list(range(half)), list(range(half, cores))]

    def device(d, q, j):
        return (d * groups + q) * cores + j

    every = [(d, q, j) for d in range(groups) for q in range(groups) for j in range(cores)]
    order = sorted(range(groups), key=lambda kd: -bin(kd).count("1"))
    got = []
    for number, slots in enumerate(phases):
        slabs = dates * (bands + 1) + (2 if number == 0 else 0)
        piece = jax.ShapeDtypeStruct((slabs, len(slots) * ROWS, LANES), jnp.bfloat16)
        pieces = pl.pallas_call(
            functools.partial(prep_kernel, groups, cores, slots, number == 0),
            out_shape=[piece] * groups,
            in_specs=[SMEM, HBM, HBM],
            out_specs=[VMEM] * groups,
            scratch_shapes=[
                pltpu.VMEM((groups, len(slots), dates) + TILE, jnp.int32),
                pltpu.SemaphoreType.DMA((groups, len(slots), bands)),
                pltpu.SemaphoreType.DMA((groups, len(slots))),
            ],
            compiler_params=params(PREP_SPARE[number]),
        )(days, stack, quality)
        moved = {0: pieces[0]}
        for kd in order:
            if kd:
                pairs = [(device(d, q, j), device(d ^ kd, q, j)) for d, q, j in every]
                moved[kd] = lax.ppermute(pieces[kd], AXES, pairs)
        got.append(moved)

    tables, fitted, totals = {}, [], None
    table = f32(dates * HARM, *TILE)
    for number, slots in enumerate(phases):
        blocks = len(slots)
        gram, moment = f32(blocks, len(PAIRS), *TILE), f32(blocks, bands * HARM, *TILE)
        weight = f32(blocks * dates, *TILE)
        far = order[0]
        steps = [[0], [kd for kd in order if kd]] if number == 0 else [[0], [far], [kd for kd in order if kd and kd != far]]
        sums, weights, done = [], {}, []
        for step, kds in enumerate(steps):
            last = step == len(steps) - 1
            inputs, outputs, scratch = {}, {}, {}
            for kd in kds:
                inputs["new.%d" % kd] = got[number][kd]
                if number == 0:
                    outputs["made.%d" % kd] = table
                else:
                    inputs["table.%d" % kd] = tables[kd]
                (scratch if last else outputs)["weight.%d" % kd] = weight
            if sums:
                inputs["in_gram"], inputs["in_moment"] = sums
            (scratch if last else outputs)["gram"] = gram
            (scratch if last else outputs)["moment"] = moment
            if number and (last or step):
                inputs["in_totals"] = totals
            if last:
                for kd in done:
                    inputs["was.%d" % kd] = got[number][kd]
                    inputs["was_table.%d" % kd] = tables[kd]
                    inputs["was_weight.%d" % kd] = weights[kd]
                for slot in slots:
                    outputs["out.%d" % slot] = f32(bands * (HARM + 1), *TILE)
                outputs["totals"] = f32(devices, LANES) if number else f32(bands + 1, *TILE)
            names = list(inputs) + list(outputs) + list(scratch)
            results = pl.pallas_call(
                functools.partial(part_kernel, (dates, bands, blocks, devices), names),
                out_shape=list(outputs.values()),
                in_specs=[VMEM] * len(inputs),
                out_specs=[VMEM] * len(outputs),
                scratch_shapes=[pltpu.VMEM(s.shape, s.dtype) for s in scratch.values()],
                compiler_params=params(24),
                cost_estimate=pl.CostEstimate(
                    flops=(200 + 200 * last * groups) * dates * blocks * ROWS * LANES * len(kds) * 8,
                    bytes_accessed=1 << 20,
                    transcendentals=0,
                ),
            )(*inputs.values())
            results = dict(zip(outputs, results, strict=True))
            for kd in kds:
                done.append(kd)
                if number == 0:
                    tables[kd] = results["made.%d" % kd]
                if not last:
                    weights[kd] = results["weight.%d" % kd]
            if last:
                fitted += [results["out.%d" % slot] for slot in slots]
                totals = results["totals"]
            else:
                sums = [results["gram"], results["moment"]]

    moved = []
    for slots in phases:
        for slot in slots:
            pairs = [(device(d, q, j), device(q, d ^ turn(groups, q, j), j ^ slot)) for d, q, j in every]
            moved.append(lax.ppermute(fitted[slot], AXES, pairs))
    totals = lax.all_to_all(totals, AXES, 0, 0, tiled=True)
    return pl.pallas_call(
        functools.partial(final_kernel, cores, bands),
        out_shape=[f32(bands, HARM, ROWS, cores * LANES), f32(bands, ROWS, cores * LANES)],
        in_specs=[VMEM] * (1 + cores),
        out_specs=[HBM, VMEM],
        scratch_shapes=[pltpu.SemaphoreType.DMA((cores, bands))],
        compiler_params=params(),
        name="final",
    )(totals, *moved)


def solution(mesh):
    groups, across = mesh.shape["date"], mesh.shape["pix"]
    cores = across // groups
    split = Mesh(mesh.devices.reshape(groups, groups, cores), AXES)

    def body(*args):
        return local(groups, cores, *args)

    return jax.shard_map(
        body,
        mesh=split,
        in_specs=(
            P("date", None, None, ("q", "j")),
            P("date", None, ("q", "j")),
            P("date"),
        ),
        out_specs=(P(None, None, ("q", "j"), "date"), P(None, ("q", "j"), "date")),
        check_vma=False,
    )
```
